8 devices in a mesh: dp: 2 (over z, y), tp: 4 (over x, core).
Axes of the slice: x: 2, y: 2, z: 1, core: 2. Of those that a mesh axis runs over, the one named last changes fastest.
Arguments:
- tokens: bfloat16 [8, 264, 1408], P('dp', 'tp')
- grad_y: bfloat16 [8, 264, 1408], P('dp', 'tp')
- valid_len: int32 [8], P('dp')
- norm1_gain: float32 [2, 1408], replicated
- norm1_bias: float32 [2, 1408], replicated
- w_qkv: bfloat16 [2, 3, 1408, 16, 88], P(None, None, None, 'tp')
- b_qkv: float32 [2, 3, 16, 88], P(None, None, 'tp')
- w_proj: bfloat16 [2, 16, 88, 1408], P(None, 'tp')
- b_proj: float32 [2, 1408], replicated
- layer_scale1: float32 [2, 1408], replicated
- norm2_gain: float32 [2, 1408], replicated
- norm2_bias: float32 [2, 1408], replicated
- w_up: bfloat16 [2, 2, 1408, 6144], P(None, None, None, 'tp')
- b_up: float32 [2, 2, 6144], P(None, None, 'tp')
- w_down: bfloat16 [2, 6144, 1408], P(None, 'tp')
- b_down: float32 [2, 1408], replicated
- layer_scale2: float32 [2, 1408], replicated
Outputs:
- output 1: bfloat16 [8, 264, 1408], P('dp', 'tp')
- output 2: bfloat16 [8, 264, 1408], P('dp', 'tp')
- output 3: float32 [2, 1408], replicated
- output 4: float32 [2, 1408], replicated
- output 5: float32 [2, 3, 1408, 16, 88], P(None, None, None, 'tp')
- output 6: float32 [2, 3, 16, 88], P(None, None, 'tp')
- output 7: float32 [2, 16, 88, 1408], P(None, 'tp')
- output 8: float32 [2, 1408], replicated
- output 9: float32 [2, 1408], replicated
- output 10: float32 [2, 1408], replicated
- output 11: float32 [2, 1408], replicated
- output 12: float32 [2, 2, 1408, 6144], P(None, None, None, 'tp')
- output 13: float32 [2, 2, 6144], P(None, None, 'tp')
- output 14: float32 [2, 6144, 1408], P(None, 'tp')
- output 15: float32 [2, 1408], replicated
- output 16: float32 [2, 1408], replicated
All inputs are finite; a program needn't handle non-finite values.
Results may differ from the reference program's by a relative error of at most 0.02.
Values are sent between devices in bfloat16 or wider.
A program may use at most 1 GiB of HBM per device.

```python
import jax
import jax.numpy as jnp
from jax import lax

WIDTH = 1408
NUM_HEADS = 16
HEAD_DIM = 88
HIDDEN = 6144
SEQ_LEN = 264
BATCH_ALL = 8
BLOCKS = 2
NORM_EPS = 1e-6
NEG_BIG = -1e9


def setup_inputs(seed: int = 0) -> dict:
    keys = jax.random.split(jax.random.key(seed), 20)
    low_len = SEQ_LEN - SEQ_LEN // 4
    row_scale = jax.random.uniform(keys[0], (BATCH_ALL, SEQ_LEN, 1), minval=0.5, maxval=2.0)
    tokens = (jax.random.normal(keys[1], (BATCH_ALL, SEQ_LEN, WIDTH)) * row_scale).astype(jnp.bfloat16)
    grad_y = jax.random.normal(keys[2], (BATCH_ALL, SEQ_LEN, WIDTH)).astype(jnp.bfloat16)
    valid_len = jax.random.randint(keys[3], (BATCH_ALL,), low_len, SEQ_LEN + 1).astype(jnp.int32)
    valid_len = valid_len.at[0].set(SEQ_LEN).at[BATCH_ALL - 1].set(low_len)
    width_scale = WIDTH ** -0.5
    vec_shape = (BLOCKS, WIDTH)
    return {
        'tokens': tokens,
        'grad_y': grad_y,
        'valid_len': valid_len,
        'norm1_gain': 1.0 + 0.25 * jax.random.normal(keys[4], vec_shape),
        'norm1_bias': 0.2 * jax.random.normal(keys[5], vec_shape),
        'w_qkv': (jax.random.normal(keys[6], (BLOCKS, 3, WIDTH, NUM_HEADS, HEAD_DIM)) * width_scale).astype(jnp.bfloat16),
        'b_qkv': 0.3 * jax.random.normal(keys[7], (BLOCKS, 3, NUM_HEADS, HEAD_DIM)),
        'w_proj': (jax.random.normal(keys[8], (BLOCKS, NUM_HEADS, HEAD_DIM, WIDTH)) * width_scale).astype(jnp.bfloat16),
        'b_proj': 0.2 * jax.random.normal(keys[9], vec_shape),
        'layer_scale1': jax.random.uniform(keys[10], vec_shape, minval=0.2, maxval=0.8),
        'norm2_gain': 1.0 + 0.25 * jax.random.normal(keys[11], vec_shape),
        'norm2_bias': 0.2 * jax.random.normal(keys[12], vec_shape),
        'w_up': (jax.random.normal(keys[13], (BLOCKS, 2, WIDTH, HIDDEN)) * width_scale).astype(jnp.bfloat16),
        'b_up': 0.3 * jax.random.normal(keys[14], (BLOCKS, 2, HIDDEN)),
        'w_down': (jax.random.normal(keys[15], (BLOCKS, HIDDEN, WIDTH)) * HIDDEN ** -0.5).astype(jnp.bfloat16),
        'b_down': 0.2 * jax.random.normal(keys[16], vec_shape),
        'layer_scale2': jax.random.uniform(keys[17], vec_shape, minval=0.2, maxval=0.8),
    }


def layer_norm(x_tok, norm_gain, norm_shift):
    x_f32 = x_tok.astype(jnp.float32)
    centered = x_f32 - jnp.mean(x_f32, axis=-1, keepdims=True)
    var_val = jnp.mean(centered * centered, axis=-1, keepdims=True)
    return centered * lax.rsqrt(var_val + NORM_EPS) * norm_gain + norm_shift


def one_block(x_seq, key_mask, layer_prm):
    (norm1_gain, norm1_bias, w_qkv, b_qkv, w_proj, b_proj, layer_scale1,
     norm2_gain, norm2_bias, w_up, b_up, w_down, b_down, layer_scale2) = layer_prm
    normed = layer_norm(x_seq, norm1_gain, norm1_bias).astype(jnp.bfloat16).astype(jnp.float32)
    qkv_heads = (jnp.einsum('nd,cdhe->cnhe', normed, w_qkv) + b_qkv[:, None]).astype(jnp.bfloat16).astype(jnp.float32)
    scores = jnp.einsum('qhe,khe->hqk', qkv_heads[0], qkv_heads[1]) * (HEAD_DIM ** -0.5)
    attn_probs = jax.nn.softmax(jnp.where(key_mask, scores, NEG_BIG), axis=-1).astype(jnp.bfloat16).astype(jnp.float32)
    attn_heads = jnp.einsum('hqk,khe->qhe', attn_probs, qkv_heads[2]).astype(jnp.bfloat16).astype(jnp.float32)
    attn_sum = jnp.einsum('qhe,hed->qd', attn_heads, w_proj) + b_proj
    x_mid = (x_seq.astype(jnp.float32) + layer_scale1 * attn_sum).astype(jnp.bfloat16)
    normed2 = layer_norm(x_mid, norm2_gain, norm2_bias).astype(jnp.bfloat16).astype(jnp.float32)
    pre_act = jnp.einsum('nd,cdf->cnf', normed2, w_up) + b_up[:, None]
    hidden = (jax.nn.silu(pre_act[0]) * pre_act[1]).astype(jnp.bfloat16).astype(jnp.float32)
    mlp_sum = jnp.dot(hidden, w_down) + b_down
    return (x_mid.astype(jnp.float32) + layer_scale2 * mlp_sum).astype(jnp.bfloat16)


def two_blocks(x_seq, key_mask, params_f32):
    def body(x_carry, layer_prm):
        return one_block(x_carry, key_mask, layer_prm), None
    return lax.scan(body, x_seq, params_f32)[0]


def reference(tokens, grad_y, valid_len, norm1_gain, norm1_bias, w_qkv, b_qkv, w_proj, b_proj, layer_scale1,
              norm2_gain, norm2_bias, w_up, b_up, w_down, b_down, layer_scale2):
    params = (norm1_gain, norm1_bias, w_qkv, b_qkv, w_proj, b_proj, layer_scale1,
              norm2_gain, norm2_bias, w_up, b_up, w_down, b_down, layer_scale2)
    params_f32 = tuple(param_arr.astype(jnp.float32) for param_arr in params)
    positions = jnp.arange(SEQ_LEN)

    def per_seq(grad_acc, seq_row):
        x_seq, dy_seq, seq_len = seq_row
        key_mask = positions < seq_len

        def forward(x_in, params_in):
            return two_blocks(x_in, key_mask, params_in)

        y_seq, pull_back = jax.vjp(forward, x_seq, params_f32)
        dx_seq, grad_params = pull_back(dy_seq)
        grad_acc = tuple(acc_arr + grad_arr for acc_arr, grad_arr in zip(grad_acc, grad_params))
        return grad_acc, (y_seq, dx_seq)

    grad_init = tuple(jnp.zeros_like(param_arr) for param_arr in params_f32)
    grad_sums, seq_outs = lax.scan(per_seq, grad_init, (tokens, grad_y, valid_len))
    return (seq_outs[0], seq_outs[1], grad_sums[0], grad_sums[1], grad_sums[2], grad_sums[3], grad_sums[4],
            grad_sums[5], grad_sums[6], grad_sums[7], grad_sums[8], grad_sums[9], grad_sums[10], grad_sums[11],
            grad_sums[12], grad_sums[13])
```

```python
import jax
import jax.numpy as jnp
from jax import lax
from jax.sharding import PartitionSpec as P

NORM_EPS = 1e-6
NEG_BIG = -1e9
F32 = jnp.float32
BF16 = jnp.bfloat16
CORE_PAIRS = ((0, 1), (1, 0), (2, 3), (3, 2))
CHIP_PAIRS = ((0, 2), (2, 0), (1, 3), (3, 1))
DP_PAIRS = ((0, 1), (1, 0))


def to_core(val):
    return lax.ppermute(val, 'tp', CORE_PAIRS)


def to_chip(val):
    return lax.ppermute(val, 'tp', CHIP_PAIRS)


def to_dp(val):
    return lax.ppermute(val, 'dp', DP_PAIRS)


def sum_all(val):
    val = val + to_core(val)
    val = val + to_chip(val)
    return val + to_dp(val)


def gather_rows(rows):
    core_rows = to_core(rows)
    chip_rows = to_chip(rows)
    diag_rows = to_core(chip_rows)
    return jnp.concatenate([rows, core_rows], 0), jnp.concatenate([chip_rows, diag_rows], 0)


def gather_other_dp(near, far):
    num = near.shape[0] // 2
    near_own = to_dp(near[:num])
    far_own = to_dp(far[:num])
    return (jnp.concatenate([near_own, to_core(near_own)], 0),
            jnp.concatenate([far_own, to_core(far_own)], 0))


def scatter_rows(part_far, part_near):
    num = part_far.shape[0] // 2
    far_sum = (part_far[:num].astype(F32) + to_core(part_far[num:]).astype(F32)).astype(BF16)
    from_chip = to_chip(far_sum)
    from_core = to_core(part_near[num:])
    return part_near[:num].astype(F32) + from_core.astype(F32) + from_chip.astype(F32)


def norm_fwd(x_rows, gain, bias):
    x_f32 = x_rows.astype(F32)
    centered = x_f32 - jnp.mean(x_f32, axis=-1, keepdims=True)
    inv_std = lax.rsqrt(jnp.mean(centered * centered, axis=-1, keepdims=True) + NORM_EPS)
    x_hat = centered * inv_std
    return (x_hat * gain + bias).astype(BF16), x_hat, inv_std


def norm_bwd(grad_out, x_hat, inv_std, gain):
    grad_hat = grad_out * gain
    mean_one = jnp.mean(grad_hat, axis=-1, keepdims=True)
    mean_two = jnp.mean(grad_hat * x_hat, axis=-1, keepdims=True)
    grad_in = inv_std * (grad_hat - mean_one - x_hat * mean_two)
    return grad_in, jnp.sum(grad_out * x_hat, axis=0), jnp.sum(grad_out, axis=0)


def dot32(spec, left, right):
    return jnp.einsum(spec, left, right, preferred_element_type=F32)


def up_fwd(rows, w_up, b_up):
    return dot32('td,cdf->ctf', rows, w_up) + b_up[:, None]


def act_fwd(pre):
    return (jax.nn.silu(pre[0]) * pre[1]).astype(BF16)


def act_bwd(grad_hidden, pre):
    gate, lin = pre[0], pre[1]
    sig = jax.nn.sigmoid(gate)
    grad_gate = grad_hidden * lin * sig * (1.0 + gate * (1.0 - sig))
    grad_lin = grad_hidden * gate * sig
    return jnp.stack([grad_gate, grad_lin])


def block_fwd(x_loc, key_mask, prm, num_seq):
    (norm1_gain, norm1_bias, w_qkv, b_qkv, w_proj, b_proj, layer_scale1,
     norm2_gain, norm2_bias, w_up, b_up, w_down, b_down, layer_scale2) = prm
    width = x_loc.shape[-1]
    heads, head_dim = b_qkv.shape[-2:]
    normed, hat_one, std_one = norm_fwd(x_loc, norm1_gain, norm1_bias)
    near, far = gather_rows(normed)
    half = near.shape[0]
    qkv = jnp.concatenate([
        (dot32('td,cdhe->cthe', rows, w_qkv) + b_qkv[:, None]).astype(BF16) for rows in (near, far)], 1)
    qkv = qkv.reshape(3, 4, num_seq, -1, heads, head_dim).transpose(0, 2, 4, 1, 3, 5)
    qkv = qkv.reshape(3, num_seq, heads, -1, head_dim)
    scores = dot32('bhqe,bhke->bhqk', qkv[0], qkv[1]) * (head_dim ** -0.5)
    probs = jax.nn.softmax(jnp.where(key_mask, scores, NEG_BIG), axis=-1)
    probs_bf = probs.astype(BF16)
    attn = dot32('bhqk,bhke->bhqe', probs_bf, qkv[2]).astype(BF16)
    attn = attn.reshape(num_seq, heads, 4, -1, head_dim).transpose(2, 0, 3, 1, 4).reshape(2 * half, heads, head_dim)
    proj_far = dot32('the,hed->td', attn[half:], w_proj).astype(BF16)
    proj_near = dot32('the,hed->td', attn[:half], w_proj).astype(BF16)
    attn_sum = scatter_rows(proj_far, proj_near) + b_proj
    x_mid = (x_loc.astype(F32) + layer_scale1 * attn_sum).astype(BF16)
    normed2, hat_two, std_two = norm_fwd(x_mid, norm2_gain, norm2_bias)
    near2, far2 = gather_rows(normed2)
    pre_near = up_fwd(near2, w_up, b_up)
    pre_far = up_fwd(far2, w_up, b_up)
    hid_far = act_fwd(pre_far)
    down_far = dot32('tf,fd->td', hid_far, w_down).astype(BF16)
    hid_near = act_fwd(pre_near)
    down_near = dot32('tf,fd->td', hid_near, w_down).astype(BF16)
    mlp_sum = scatter_rows(down_far, down_near) + b_down
    x_out = (x_mid.astype(F32) + layer_scale2 * mlp_sum).astype(BF16)
    saved = (hat_one, std_one, near, far, qkv, probs, probs_bf, attn, attn_sum,
             hat_two, std_two, near2, far2, pre_near, pre_far, hid_near, hid_far, mlp_sum)
    return x_out, saved


def block_bwd(grad_x, saved, prm, num_seq):
    (norm1_gain, norm1_bias, w_qkv, b_qkv, w_proj, b_proj, layer_scale1,
     norm2_gain, norm2_bias, w_up, b_up, w_down, b_down, layer_scale2) = prm
    (hat_one, std_one, near, far, qkv, probs, probs_bf, attn, attn_sum,
     hat_two, std_two, near2, far2, pre_near, pre_far, hid_near, hid_far, mlp_sum) = saved
    heads, head_dim = b_qkv.shape[-2:]
    half = near.shape[0]
    grad_res = grad_x.astype(F32)
    grad_ls2 = jnp.sum(grad_res * mlp_sum, axis=0)
    grad_mlp = layer_scale2 * grad_res
    grad_b_down = jnp.sum(grad_mlp, axis=0)
    gm_near, gm_far = gather_rows(grad_mlp.astype(BF16))
    gp_near = act_bwd(dot32('td,fd->tf', gm_near, w_down), pre_near)
    gp_far = act_bwd(dot32('td,fd->tf', gm_far, w_down), pre_far)
    gpb_near = gp_near.astype(BF16)
    gpb_far = gp_far.astype(BF16)
    n2_far = dot32('ctf,cdf->td', gpb_far, w_up).astype(BF16)
    n2_near = dot32('ctf,cdf->td', gpb_near, w_up).astype(BF16)
    grad_normed2 = scatter_rows(n2_far, n2_near)
    grad_b_up = jnp.sum(gp_near, axis=1) + jnp.sum(gp_far, axis=1)
    grad_b_up = grad_b_up + to_dp(grad_b_up)
    on_near, on_far = gather_other_dp(near2, far2)
    og_near, og_far = gather_other_dp(gm_near, gm_far)
    ohid, ogp = [], []
    for rows, grads in ((on_near, og_near), (on_far, og_far)):
        pre = up_fwd(rows, w_up, b_up)
        ohid.append(act_fwd(pre))
        ogp.append(act_bwd(dot32('td,fd->tf', grads, w_down), pre).astype(BF16))
    gm_all = jnp.concatenate([gm_near, gm_far, og_near, og_far], 0)
    hid_all = jnp.concatenate([hid_near, hid_far] + ohid, 0)
    gp_all = jnp.concatenate([gpb_near, gpb_far] + ogp, 1)
    n2_all = jnp.concatenate([near2, far2, on_near, on_far], 0)
    grad_w_down = dot32('tf,td->fd', hid_all, gm_all)
    grad_w_up = dot32('td,ctf->cdf', n2_all, gp_all)

    grad_from2, grad_n2g, grad_n2b = norm_bwd(grad_normed2, hat_two, std_two, norm2_gain)
    grad_mid = grad_res + grad_from2
    grad_ls1 = jnp.sum(grad_mid * attn_sum, axis=0)
    grad_attn_out = layer_scale1 * grad_mid
    grad_b_proj = jnp.sum(grad_attn_out, axis=0)
    ga_near, ga_far = gather_rows(grad_attn_out.astype(BF16))
    grad_attn = jnp.concatenate(
        [dot32('td,hed->the', rows, w_proj).astype(BF16) for rows in (ga_near, ga_far)], 0)
    ga_all = jnp.concatenate([ga_near, ga_far], 0)
    grad_w_proj = dot32('the,td->hed', attn, ga_all).astype(BF16)
    grad_w_proj = grad_w_proj.astype(F32) + to_dp(grad_w_proj).astype(F32)
    grad_attn = grad_attn.reshape(4, num_seq, -1, heads, head_dim).transpose(1, 3, 0, 2, 4)
    grad_attn = grad_attn.reshape(num_seq, heads, -1, head_dim)
    grad_probs = dot32('bhqe,bhke->bhqk', grad_attn, qkv[2])
    grad_val = dot32('bhqk,bhqe->bhke', probs_bf, grad_attn)
    grad_scores = (probs * (grad_probs - jnp.sum(grad_probs * probs, axis=-1, keepdims=True))
                   * (head_dim ** -0.5)).astype(BF16)
    grad_query = dot32('bhqk,bhke->bhqe', grad_scores, qkv[1])
    grad_key = dot32('bhqk,bhqe->bhke', grad_scores, qkv[0])
    grad_qkv = jnp.stack([grad_query, grad_key, grad_val])
    grad_b_qkv = jnp.sum(grad_qkv, axis=(1, 3))
    grad_b_qkv = grad_b_qkv + to_dp(grad_b_qkv)
    grad_qkv = grad_qkv.astype(BF16).reshape(3, num_seq, heads, 4, -1, head_dim).transpose(0, 3, 1, 4, 2, 5)
    grad_qkv = grad_qkv.reshape(3, 2 * half, heads, head_dim)
    n1_far = dot32('cthe,cdhe->td', grad_qkv[:, half:], w_qkv).astype(BF16)
    n1_near = dot32('cthe,cdhe->td', grad_qkv[:, :half], w_qkv).astype(BF16)
    grad_normed = scatter_rows(n1_far, n1_near)
    n1_all = jnp.concatenate([near, far], 0)
    grad_w_qkv = dot32('td,cthe->cdhe', n1_all, grad_qkv).astype(BF16)
    grad_w_qkv = grad_w_qkv.astype(F32) + to_dp(grad_w_qkv).astype(F32)
    grad_from1, grad_n1g, grad_n1b = norm_bwd(grad_normed, hat_one, std_one, norm1_gain)
    grad_in = (grad_mid + grad_from1).astype(BF16)
    shared = sum_all(jnp.stack([grad_n1g, grad_n1b, grad_b_proj, grad_ls1, grad_n2g, grad_n2b, grad_b_down, grad_ls2]))
    layer_grads = (shared[0], shared[1], grad_w_qkv, grad_b_qkv, grad_w_proj, shared[2], shared[3],
                   shared[4], shared[5], grad_w_up, grad_b_up, grad_w_down, shared[6], shared[7])
    return grad_in, layer_grads


def solution(mesh):
    small_spec = P()
    act_spec = P('dp', 'tp', None)
    param_specs = (small_spec, small_spec, P(None, None, None, 'tp', None), P(None, None, 'tp', None),
                   P(None, 'tp', None, None), small_spec, small_spec, small_spec, small_spec,
                   P(None, None, None, 'tp'), P(None, None, 'tp'), P(None, 'tp', None), small_spec, small_spec)

    def device_fn(tokens, grad_y, valid_len, *params):
        num_blocks = params[0].shape[0]
        num_seq, num_tok, width = tokens.shape
        slots = lax.axis_index('tp') ^ jnp.arange(4)
        positions = (slots[:, None] * num_tok + jnp.arange(num_tok)[None, :]).reshape(-1)
        key_mask = (positions[None, :] < valid_len[:, None])[:, None, None, :]
        x_cur = tokens.reshape(num_seq * num_tok, width)
        saved_all = []
        for layer_idx in range(num_blocks):
            x_cur, saved = block_fwd(x_cur, key_mask, tuple(arr[layer_idx] for arr in params), num_seq)
            saved_all.append(saved)
        grad_cur = grad_y.reshape(num_seq * num_tok, width)
        grads_rev = []
        for layer_idx in reversed(range(num_blocks)):
            grad_cur, layer_grads = block_bwd(grad_cur, saved_all[layer_idx],
                                              tuple(arr[layer_idx] for arr in params), num_seq)
            grads_rev.append(layer_grads)
        grads_fwd = grads_rev[::-1]
        stacked = [jnp.stack([one[slot] for one in grads_fwd]) for slot in range(len(params))]
        return (x_cur.reshape(tokens.shape), grad_cur.reshape(tokens.shape)) + tuple(stacked)

    return jax.shard_map(device_fn, mesh=mesh, in_specs=(act_spec, act_spec, P('dp')) + param_specs,
                         out_specs=(act_spec, act_spec) + param_specs, check_vma=False)
```

```python
import functools

import jax
import jax.numpy as jnp
from jax import lax
from jax.experimental import pallas as pl
from jax.experimental.pallas import tpu as pltpu
from jax.sharding import PartitionSpec as P

NORM_EPS = 1e-6
NEG_BIG = -1e9
F32 = jnp.float32
BF16 = jnp.bfloat16
CORE_PAIRS = ((0, 1), (1, 0), (2, 3), (3, 2))
CHIP_PAIRS = ((0, 2), (2, 0), (1, 3), (3, 1))
DP_PAIRS = ((0, 1), (1, 0))


def to_core(val):
    return lax.ppermute(val, 'tp', CORE_PAIRS)


def to_chip(val):
    return lax.ppermute(val, 'tp', CHIP_PAIRS)


def to_dp(val):
    return lax.ppermute(val, 'dp', DP_PAIRS)


def sum_all(val):
    val = val + to_core(val)
    val = val + to_chip(val)
    return val + to_dp(val)


def gather_rows(rows):
    core_rows = to_core(rows)
    chip_rows = to_chip(rows)
    diag_rows = to_core(chip_rows)
    return jnp.concatenate([rows, core_rows], 0), jnp.concatenate([chip_rows, diag_rows], 0)


def gather_other_dp(near, far):
    num = near.shape[0] // 2
    near_own = to_dp(near[:num])
    far_own = to_dp(far[:num])
    return (jnp.concatenate([near_own, to_core(near_own)], 0),
            jnp.concatenate([far_own, to_core(far_own)], 0))


def scatter_rows(part_far, part_near):
    num = part_far.shape[0] // 2
    far_sum = (part_far[:num].astype(F32) + to_core(part_far[num:]).astype(F32)).astype(BF16)
    from_chip = to_chip(far_sum)
    from_core = to_core(part_near[num:])
    return part_near[:num].astype(F32) + from_core.astype(F32) + from_chip.astype(F32)


def norm_fwd(x_rows, gain, bias):
    x_f32 = x_rows.astype(F32)
    centered = x_f32 - jnp.mean(x_f32, axis=-1, keepdims=True)
    inv_std = lax.rsqrt(jnp.mean(centered * centered, axis=-1, keepdims=True) + NORM_EPS)
    x_hat = centered * inv_std
    return (x_hat * gain + bias).astype(BF16), x_hat, inv_std


def norm_bwd(grad_out, x_hat, inv_std, gain):
    grad_hat = grad_out * gain
    mean_one = jnp.mean(grad_hat, axis=-1, keepdims=True)
    mean_two = jnp.mean(grad_hat * x_hat, axis=-1, keepdims=True)
    grad_in = inv_std * (grad_hat - mean_one - x_hat * mean_two)
    return grad_in, jnp.sum(grad_out * x_hat, axis=0), jnp.sum(grad_out, axis=0)


def dot32(spec, left, right):
    return jnp.einsum(spec, left, right, preferred_element_type=F32)


WGRAD_PARTS = 2
VMEM_BYTES = 60 * 1024 * 1024


def row_chunks(num_rows):
    step = num_rows // 2
    return [slice(start, start + step) for start in range(0, num_rows, step)]


def dot_nn(left, right):
    return lax.dot_general(left, right, (((1,), (0,)), ((), ())), preferred_element_type=F32)


def dot_nt(left, right):
    return lax.dot_general(left, right, (((1,), (1,)), ((), ())), preferred_element_type=F32)


def dot_tn(left, right):
    return lax.dot_general(left, right, (((0,), (0,)), ((), ())), preferred_element_type=F32)


def act_grads(grad_hidden, gate, lin, sig):
    gated = gate * sig
    return grad_hidden * lin * (sig * (1.0 + gate * (1.0 - sig))), grad_hidden * gated


def mlp_fwd_kernel(x_ref, wu_ref, bu_ref, wd_ref, pre_ref, hid_ref, part_ref, acc_ref):
    step, last = pl.program_id(0), pl.num_programs(0) - 1
    for rows in row_chunks(x_ref.shape[0]):
        x_rows = x_ref[rows, :]
        gate = dot_nn(x_rows, wu_ref[0, 0]) + bu_ref[0, 0:1, :]
        lin = dot_nn(x_rows, wu_ref[0, 1]) + bu_ref[0, 1:2, :]
        pre_ref[0, rows, :] = gate
        pre_ref[1, rows, :] = lin
        hid = (gate * jax.nn.sigmoid(gate) * lin).astype(BF16)
        hid_ref[rows, :] = hid
        part = dot_nn(hid, wd_ref[0])

        @pl.when(step == 0)
        def _():
            acc_ref[rows, :] = part

        @pl.when(step > 0)
        def _():
            acc_ref[rows, :] += part

    @pl.when(step == last)
    def _():
        part_ref[...] = acc_ref[...].astype(BF16)


def mlp_fwd(rows, w_up, b_up, w_down, layer, tile=512):
    num, width = rows.shape
    hidden = w_up.shape[-1]
    return pl.pallas_call(
        mlp_fwd_kernel,
        grid=(hidden // tile,),
        in_specs=[pl.BlockSpec((num, width), lambda f: (0, 0)),
                  pl.BlockSpec((1, 2, width, tile), lambda f: (layer, 0, 0, f)),
                  pl.BlockSpec((1, 2, tile), lambda f: (layer, 0, f)),
                  pl.BlockSpec((1, tile, width), lambda f: (layer, f, 0))],
        out_specs=[pl.BlockSpec((2, num, tile), lambda f: (0, 0, f)),
                   pl.BlockSpec((num, tile), lambda f: (0, f)),
                   pl.BlockSpec((num, width), lambda f: (0, 0))],
        out_shape=[jax.ShapeDtypeStruct((2, num, hidden), F32),
                   jax.ShapeDtypeStruct((num, hidden), BF16),
                   jax.ShapeDtypeStruct((num, width), BF16)],
        scratch_shapes=[pltpu.VMEM((num, width), F32)],
        compiler_params=pltpu.CompilerParams(vmem_limit_bytes=VMEM_BYTES),
        cost_estimate=pl.CostEstimate(flops=6 * num * width * hidden, bytes_accessed=6 * width * hidden,
                                      transcendentals=num * hidden),
        name='mlp_fwd',
    )(rows, w_up, b_up, w_down)


def mlp_bwd_kernel(gm_ref, pre_ref, wu_ref, wd_ref, gp_ref, part_ref, bsum_ref, acc_ref):
    step, last = pl.program_id(0), pl.num_programs(0) - 1
    sums = []
    for rows in row_chunks(gm_ref.shape[0]):
        grad_hidden = dot_nt(gm_ref[rows, :], wd_ref[0])
        gate, lin = pre_ref[0, rows, :], pre_ref[1, rows, :]
        grad_gate, grad_lin = act_grads(grad_hidden, gate, lin, jax.nn.sigmoid(gate))
        sums.append((jnp.sum(grad_gate, axis=0, keepdims=True), jnp.sum(grad_lin, axis=0, keepdims=True)))
        grad_gate, grad_lin = grad_gate.astype(BF16), grad_lin.astype(BF16)
        gp_ref[0, rows, :] = grad_gate
        gp_ref[1, rows, :] = grad_lin
        part = dot_nt(grad_gate, wu_ref[0, 0]) + dot_nt(grad_lin, wu_ref[0, 1])

        @pl.when(step == 0)
        def _():
            acc_ref[rows, :] = part

        @pl.when(step > 0)
        def _():
            acc_ref[rows, :] += part

    bsum_ref[0:1, :] = sums[0][0] + sums[1][0]
    bsum_ref[1:2, :] = sums[0][1] + sums[1][1]

    @pl.when(step == last)
    def _():
        part_ref[...] = acc_ref[...].astype(BF16)


def mlp_bwd(grads, pre, w_up, w_down, layer, tile=512):
    num, width = grads.shape
    hidden = w_up.shape[-1]
    return pl.pallas_call(
        mlp_bwd_kernel,
        grid=(hidden // tile,),
        in_specs=[pl.BlockSpec((num, width), lambda f: (0, 0)),
                  pl.BlockSpec((2, num, tile), lambda f: (0, 0, f)),
                  pl.BlockSpec((1, 2, width, tile), lambda f: (layer, 0, 0, f)),
                  pl.BlockSpec((1, tile, width), lambda f: (layer, f, 0))],
        out_specs=[pl.BlockSpec((2, num, tile), lambda f: (0, 0, f)),
                   pl.BlockSpec((num, width), lambda f: (0, 0)),
                   pl.BlockSpec((2, tile), lambda f: (0, f))],
        out_shape=[jax.ShapeDtypeStruct((2, num, hidden), BF16),
                   jax.ShapeDtypeStruct((num, width), BF16),
                   jax.ShapeDtypeStruct((2, hidden), F32)],
        scratch_shapes=[pltpu.VMEM((num, width), F32)],
        compiler_params=pltpu.CompilerParams(vmem_limit_bytes=VMEM_BYTES),
        cost_estimate=pl.CostEstimate(flops=6 * num * width * hidden, bytes_accessed=6 * width * hidden,
                                      transcendentals=num * hidden),
        name='mlp_bwd',
    )(grads, pre, w_up, w_down)


def mlp_wgrad_kernel(num_alias, xt_hbm, gmn_hbm, gmf_hbm, ogn_hbm, ogf_hbm, xn_ref, xf_ref, wu_ref, bu_ref, wd_ref,
                     hn_ref, hf_ref, gpn_ref, gpf_ref, *rest):
    gwu_ref, gwd_ref, xt_ref, gm_ref, hid_ref, gp_ref, sems = rest[num_alias:]
    num = xn_ref.shape[0]
    copies = [pltpu.make_async_copy(src, gm_ref.at[pl.ds(pos * num, num), :], sems.at[pos])
              for pos, src in ((2, ogn_hbm), (3, ogf_hbm), (0, gmn_hbm), (1, gmf_hbm))]
    copies.append(pltpu.make_async_copy(xt_hbm, xt_ref, sems.at[4]))
    first = pl.program_id(0) == 0

    @pl.when(first)
    def _():
        for copy in copies:
            copy.start()

    hid_ref[0:num, :] = hn_ref[...]
    hid_ref[num:2 * num, :] = hf_ref[...]
    for chan in range(2):
        gp_ref[chan, 0:num, :] = gpn_ref[chan]
        gp_ref[chan, num:2 * num, :] = gpf_ref[chan]

    @pl.when(first)
    def _():
        for copy in copies[:2]:
            copy.wait()

    for pos, x_ref in ((2, xn_ref), (3, xf_ref)):
        x_rows = x_ref[...]
        rows = slice(pos * num, (pos + 1) * num)
        gate = dot_nn(x_rows, wu_ref[0, 0]) + bu_ref[0, 0:1, :]
        lin = dot_nn(x_rows, wu_ref[0, 1]) + bu_ref[0, 1:2, :]
        grad_hidden = dot_nt(gm_ref[rows, :], wd_ref[0])
        sig = jax.nn.sigmoid(gate)
        hid_ref[rows, :] = (gate * sig * lin).astype(BF16)
        grad_gate, grad_lin = act_grads(grad_hidden, gate, lin, sig)
        gp_ref[0, rows, :] = grad_gate.astype(BF16)
        gp_ref[1, rows, :] = grad_lin.astype(BF16)

    @pl.when(first)
    def _():
        for copy in copies[2:]:
            copy.wait()

    for chan in range(2):
        gwu_ref[0, chan] = dot_nn(xt_ref[...], gp_ref[chan])
    gwd_ref[0] = dot_tn(hid_ref[...], gm_ref[...])


def mlp_wgrad(part, num_parts, layer, bufs, xt_all, gm_own, gm_other, x_other, w_up, b_up, w_down, hid, gp, tile=256):
    width, tokens = xt_all.shape
    num = tokens // 4
    hidden = w_up.shape[-1]
    steps = hidden // tile // num_parts
    base = part * steps
    any_spec = pl.BlockSpec(memory_space=pl.ANY)
    flops = 2 * width * tile * steps * (3 * 2 * num + 3 * tokens)
    return pl.pallas_call(
        functools.partial(mlp_wgrad_kernel, len(bufs)),
        grid=(steps,),
        in_specs=[any_spec] * 5 + [
            pl.BlockSpec((num, width), lambda f: (0, 0)),
            pl.BlockSpec((num, width), lambda f: (0, 0)),
            pl.BlockSpec((1, 2, width, tile), lambda f: (layer, 0, 0, f + base)),
            pl.BlockSpec((1, 2, tile), lambda f: (layer, 0, f + base)),
            pl.BlockSpec((1, tile, width), lambda f: (layer, f + base, 0)),
            pl.BlockSpec((num, tile), lambda f: (0, f + base)),
            pl.BlockSpec((num, tile), lambda f: (0, f + base)),
            pl.BlockSpec((2, num, tile), lambda f: (0, 0, f + base)),
            pl.BlockSpec((2, num, tile), lambda f: (0, 0, f + base))] + [any_spec] * len(bufs),
        out_specs=[pl.BlockSpec((1, 2, width, tile), lambda f: (layer, 0, 0, f + base)),
                   pl.BlockSpec((1, tile, width), lambda f: (layer, f + base, 0))],
        out_shape=[jax.ShapeDtypeStruct(w_up.shape, F32), jax.ShapeDtypeStruct(w_down.shape, F32)],
        input_output_aliases={14 + pos: pos for pos in range(len(bufs))},
        scratch_shapes=[pltpu.VMEM((width, tokens), BF16), pltpu.VMEM((tokens, width), BF16),
                        pltpu.VMEM((tokens, tile), BF16), pltpu.VMEM((2, tokens, tile), BF16),
                        pltpu.SemaphoreType.DMA((5,))],
        compiler_params=pltpu.CompilerParams(vmem_limit_bytes=VMEM_BYTES),
        cost_estimate=pl.CostEstimate(flops=flops, bytes_accessed=18 * width * tile * steps + 4 * tokens * width,
                                      transcendentals=2 * num * tile * steps),
        name='mlp_wgrad',
    )(xt_all, *gm_own, *gm_other, *x_other, w_up, b_up, w_down, *hid, *gp, *bufs)


def block_fwd(x_loc, key_mask, prm, layer, params, num_seq):
    (norm1_gain, norm1_bias, w_qkv, b_qkv, w_proj, b_proj, layer_scale1,
     norm2_gain, norm2_bias, w_up, b_up, w_down, b_down, layer_scale2) = prm
    width = x_loc.shape[-1]
    heads, head_dim = b_qkv.shape[-2:]
    normed, hat_one, std_one = norm_fwd(x_loc, norm1_gain, norm1_bias)
    near, far = gather_rows(normed)
    half = near.shape[0]
    qkv = jnp.concatenate([
        (dot32('td,cdhe->cthe', rows, w_qkv) + b_qkv[:, None]).astype(BF16) for rows in (near, far)], 1)
    qkv = qkv.reshape(3, 4, num_seq, -1, heads, head_dim).transpose(0, 2, 4, 1, 3, 5)
    qkv = qkv.reshape(3, num_seq, heads, -1, head_dim)
    scores = dot32('bhqe,bhke->bhqk', qkv[0], qkv[1]) * (head_dim ** -0.5)
    probs = jax.nn.softmax(jnp.where(key_mask, scores, NEG_BIG), axis=-1)
    probs_bf = probs.astype(BF16)
    attn = dot32('bhqk,bhke->bhqe', probs_bf, qkv[2]).astype(BF16)
    attn = attn.reshape(num_seq, heads, 4, -1, head_dim).transpose(2, 0, 3, 1, 4).reshape(2 * half, heads, head_dim)
    proj_far = dot32('the,hed->td', attn[half:], w_proj).astype(BF16)
    proj_near = dot32('the,hed->td', attn[:half], w_proj).astype(BF16)
    attn_sum = scatter_rows(proj_far, proj_near) + b_proj
    x_mid = (x_loc.astype(F32) + layer_scale1 * attn_sum).astype(BF16)
    normed2, hat_two, std_two = norm_fwd(x_mid, norm2_gain, norm2_bias)
    near2, far2 = gather_rows(normed2)
    mlp_params = (params[9], params[10], params[11])
    pre_near, hid_near, down_near = mlp_fwd(near2, *mlp_params, layer)
    pre_far, hid_far, down_far = mlp_fwd(far2, *mlp_params, layer)
    mlp_sum = scatter_rows(down_far, down_near) + b_down
    x_out = (x_mid.astype(F32) + layer_scale2 * mlp_sum).astype(BF16)
    saved = (hat_one, std_one, near, far, qkv, probs, probs_bf, attn, attn_sum,
             hat_two, std_two, near2, far2, pre_near, pre_far, hid_near, hid_far, mlp_sum)
    return x_out, saved


def block_bwd(grad_x, saved, prm, layer, params, bufs, num_seq):
    (norm1_gain, norm1_bias, w_qkv, b_qkv, w_proj, b_proj, layer_scale1,
     norm2_gain, norm2_bias, w_up, b_up, w_down, b_down, layer_scale2) = prm
    (hat_one, std_one, near, far, qkv, probs, probs_bf, attn, attn_sum,
     hat_two, std_two, near2, far2, pre_near, pre_far, hid_near, hid_far, mlp_sum) = saved
    heads, head_dim = b_qkv.shape[-2:]
    half = near.shape[0]
    grad_res = grad_x.astype(F32)
    grad_ls2 = jnp.sum(grad_res * mlp_sum, axis=0)
    grad_mlp = layer_scale2 * grad_res
    grad_b_down = jnp.sum(grad_mlp, axis=0)
    gm_near, gm_far = gather_rows(grad_mlp.astype(BF16))
    gpb_far, n2_far, bsum_far = mlp_bwd(gm_far, pre_far, params[9], params[11], layer)
    gpb_near, n2_near, bsum_near = mlp_bwd(gm_near, pre_near, params[9], params[11], layer)
    grad_normed2 = scatter_rows(n2_far, n2_near)
    grad_b_up = bsum_near + bsum_far
    on_near, on_far = gather_other_dp(near2, far2)
    og_near, og_far = gather_other_dp(gm_near, gm_far)
    xt_all = jnp.concatenate([near2, far2, on_near, on_far], 0).T
    for part in range(WGRAD_PARTS):
        bufs = mlp_wgrad(part, WGRAD_PARTS, layer, bufs, xt_all, (gm_near, gm_far), (og_near, og_far), (on_near, on_far),
                         params[9], params[10], params[11], (hid_near, hid_far), (gpb_near, gpb_far))

    grad_from2, grad_n2g, grad_n2b = norm_bwd(grad_normed2, hat_two, std_two, norm2_gain)
    grad_mid = grad_res + grad_from2
    grad_ls1 = jnp.sum(grad_mid * attn_sum, axis=0)
    grad_attn_out = layer_scale1 * grad_mid
    grad_b_proj = jnp.sum(grad_attn_out, axis=0)
    ga_near, ga_far = gather_rows(grad_attn_out.astype(BF16))
    grad_attn = jnp.concatenate(
        [dot32('td,hed->the', rows, w_proj).astype(BF16) for rows in (ga_near, ga_far)], 0)
    ga_all = jnp.concatenate([ga_near, ga_far], 0)
    grad_w_proj = dot32('the,td->hed', attn, ga_all).astype(BF16)
    grad_w_proj = grad_w_proj.astype(F32) + to_dp(grad_w_proj).astype(F32)
    grad_attn = grad_attn.reshape(4, num_seq, -1, heads, head_dim).transpose(1, 3, 0, 2, 4)
    grad_attn = grad_attn.reshape(num_seq, heads, -1, head_dim)
    grad_probs = dot32('bhqe,bhke->bhqk', grad_attn, qkv[2])
    grad_val = dot32('bhqk,bhqe->bhke', probs_bf, grad_attn)
    grad_scores = (probs * (grad_probs - jnp.sum(grad_probs * probs, axis=-1, keepdims=True))
                   * (head_dim ** -0.5)).astype(BF16)
    grad_scores = lax.optimization_barrier(grad_scores)
    grad_query = dot32('bhqk,bhke->bhqe', grad_scores, qkv[1])
    grad_key = dot32('bhqk,bhqe->bhke', grad_scores, qkv[0])
    grad_qkv = jnp.stack([grad_query, grad_key, grad_val])
    grad_b_qkv = jnp.sum(grad_qkv, axis=(1, 3))
    grad_qkv = grad_qkv.astype(BF16).reshape(3, num_seq, heads, 4, -1, head_dim).transpose(0, 3, 1, 4, 2, 5)
    grad_qkv = grad_qkv.reshape(3, 2 * half, heads, head_dim)
    n1_far = dot32('cthe,cdhe->td', grad_qkv[:, half:], w_qkv).astype(BF16)
    n1_near = dot32('cthe,cdhe->td', grad_qkv[:, :half], w_qkv).astype(BF16)
    grad_normed = scatter_rows(n1_far, n1_near)
    n1_all = jnp.concatenate([near, far], 0)
    grad_w_qkv = dot32('td,cthe->cdhe', n1_all, grad_qkv).astype(BF16)
    grad_w_qkv = grad_w_qkv.astype(F32) + to_dp(grad_w_qkv).astype(F32)
    grad_from1, grad_n1g, grad_n1b = norm_bwd(grad_normed, hat_one, std_one, norm1_gain)
    grad_in = (grad_mid + grad_from1).astype(BF16)
    shared = jnp.stack([grad_n1g, grad_n1b, grad_b_proj, grad_ls1, grad_n2g, grad_n2b, grad_b_down, grad_ls2])
    return grad_in, bufs, (shared, grad_b_qkv, grad_b_up, grad_w_qkv, grad_w_proj)


def solution(mesh):
    small_spec = P()
    act_spec = P('dp', 'tp', None)
    param_specs = (small_spec, small_spec, P(None, None, None, 'tp', None), P(None, None, 'tp', None),
                   P(None, 'tp', None, None), small_spec, small_spec, small_spec, small_spec,
                   P(None, None, None, 'tp'), P(None, None, 'tp'), P(None, 'tp', None), small_spec, small_spec)

    def device_fn(tokens, grad_y, valid_len, *params):
        num_blocks = params[0].shape[0]
        num_seq, num_tok, width = tokens.shape
        slots = lax.axis_index('tp') ^ jnp.arange(4)
        positions = (slots[:, None] * num_tok + jnp.arange(num_tok)[None, :]).reshape(-1)
        key_mask = (positions[None, :] < valid_len[:, None])[:, None, None, :]
        x_cur = tokens.reshape(num_seq * num_tok, width)
        saved_all = []
        for layer in range(num_blocks):
            x_cur, saved = block_fwd(x_cur, key_mask, tuple(arr[layer] for arr in params), layer, params, num_seq)
            saved_all.append(saved)
        grad_cur = grad_y.reshape(num_seq * num_tok, width)
        grads = [None] * num_blocks
        bufs = ()
        for layer in reversed(range(num_blocks)):
            grad_cur, bufs, grads[layer] = block_bwd(grad_cur, saved_all[layer], tuple(arr[layer] for arr in params),
                                                     layer, params, bufs, num_seq)
        shared, b_qkv, b_up, w_qkv, w_proj = (jnp.stack(vals) for vals in zip(*grads))
        b_qkv, b_up = b_qkv + to_dp(b_qkv), b_up + to_dp(b_up)
        shared = sum_all(shared.reshape(-1, width)).reshape(num_blocks, -1, width).transpose(1, 0, 2)
        return (x_cur.reshape(tokens.shape), grad_cur.reshape(tokens.shape), shared[0], shared[1], w_qkv, b_qkv,
                w_proj, shared[2], shared[3], shared[4], shared[5], bufs[0], b_up, bufs[1], shared[6], shared[7])

    return jax.shard_map(device_fn, mesh=mesh, in_specs=(act_spec, act_spec, P('dp')) + param_specs,
                         out_specs=(act_spec, act_spec) + param_specs, check_vma=False)
```

```python
import functools

import jax
import jax.numpy as jnp
from jax import lax
from jax.experimental import pallas as pl
from jax.experimental.pallas import tpu as pltpu
from jax.sharding import PartitionSpec as P

NORM_EPS = 1e-6
NEG_BIG = -1e9
F32 = jnp.float32
BF16 = jnp.bfloat16
CORE_PAIRS = ((0, 1), (1, 0), (2, 3), (3, 2))
CHIP_PAIRS = ((0, 2), (2, 0), (1, 3), (3, 1))
DP_PAIRS = ((0, 1), (1, 0))


def to_core(val):
    return lax.ppermute(val, 'tp', CORE_PAIRS)


def to_chip(val):
    return lax.ppermute(val, 'tp', CHIP_PAIRS)


def to_dp(val):
    return lax.ppermute(val, 'dp', DP_PAIRS)


def sum_all(val):
    val = val + to_core(val)
    val = val + to_chip(val)
    return val + to_dp(val)


def gather_rows(rows, token_fn=None):
    core_rows = to_core(rows)
    chip_rows = to_chip(rows)
    if token_fn is not None:
        chip_rows = after_token(chip_rows, token_fn(rows))
    diag_rows = to_core(chip_rows)
    return jnp.concatenate([rows, core_rows], 0), jnp.concatenate([chip_rows, diag_rows], 0)


def gather_other_dp(near, far):
    num = near.shape[0] // 2
    near_own = to_dp(near[:num])
    far_own = to_dp(far[:num])
    return (jnp.concatenate([near_own, to_core(near_own)], 0),
            jnp.concatenate([far_own, to_core(far_own)], 0))


def scatter_rows(parts, token_fn=None):
    far_sum = (parts[2].astype(F32) + to_core(parts[3]).astype(F32)).astype(BF16)
    from_chip = to_chip(far_sum)
    from_core = to_core(parts[1])
    if token_fn is not None:
        from_chip = after_token(from_chip, token_fn(far_sum))
    return parts[0].astype(F32) + from_core.astype(F32) + from_chip.astype(F32)


def after_token(val, token):
    return lax.optimization_barrier((val, token))[0]


def norm_fwd(x_rows, gain, bias):
    x_f32 = x_rows.astype(F32)
    centered = x_f32 - jnp.mean(x_f32, axis=-1, keepdims=True)
    inv_std = lax.rsqrt(jnp.mean(centered * centered, axis=-1, keepdims=True) + NORM_EPS)
    x_hat = centered * inv_std
    return (x_hat * gain + bias).astype(BF16), x_hat, inv_std


def norm_bwd(grad_out, x_hat, inv_std, gain):
    grad_hat = grad_out * gain
    mean_one = jnp.mean(grad_hat, axis=-1, keepdims=True)
    mean_two = jnp.mean(grad_hat * x_hat, axis=-1, keepdims=True)
    grad_in = inv_std * (grad_hat - mean_one - x_hat * mean_two)
    return grad_in, jnp.sum(grad_out * x_hat, axis=0), jnp.sum(grad_out, axis=0)


WGRAD_PARTS = 3
LANES = 128
SEQ_WINDOW = 80
LOW_FILL = -3e38
VMEM_BYTES = 60 * 1024 * 1024


def dot_nn(left, right):
    return lax.dot_general(left, right, (((1,), (0,)), ((), ())), preferred_element_type=F32)


def dot_nt(left, right):
    return lax.dot_general(left, right, (((1,), (1,)), ((), ())), preferred_element_type=F32)


def dot_tn(left, right):
    return lax.dot_general(left, right, (((0,), (0,)), ((), ())), preferred_element_type=F32)


def act_grads(grad_hidden, gate, lin, sig):
    gated = gate * sig
    return grad_hidden * lin * (sig * (1.0 + gate * (1.0 - sig))), grad_hidden * gated


def join_rows(near_ref, far_ref, all_ref):
    num = near_ref.shape[0]
    all_ref[0:num, :] = near_ref[...]
    all_ref[num:2 * num, :] = far_ref[...]


def add_into(acc_ref, val, first):
    @pl.when(first)
    def _():
        acc_ref[...] = val

    @pl.when(jnp.logical_not(first))
    def _():
        acc_ref[...] += val


def store_parts(acc_ref, part_refs):
    num = acc_ref.shape[0] // 4
    for pos, part_ref in enumerate(part_refs):
        part_ref[...] = acc_ref[pos * num:(pos + 1) * num, :].astype(BF16)


def whole(shape):
    return pl.BlockSpec(shape, lambda f: (0,) * len(shape))


def mlp_fwd_kernel(near_ref, far_ref, wu_ref, bu_ref, wd_ref, pre_ref, hid_ref, p0, p1, p2, p3, x_ref, acc_ref):
    step, last = pl.program_id(0), pl.num_programs(0) - 1

    @pl.when(step == 0)
    def _():
        join_rows(near_ref, far_ref, x_ref)

    gate = dot_nn(x_ref[...], wu_ref[0, 0]) + bu_ref[0, 0:1, :]
    lin = dot_nn(x_ref[...], wu_ref[0, 1]) + bu_ref[0, 1:2, :]
    pre_ref[0] = gate
    pre_ref[1] = lin
    hid = (gate * jax.nn.sigmoid(gate) * lin).astype(BF16)
    hid_ref[...] = hid
    add_into(acc_ref, dot_nn(hid, wd_ref[0]), step == 0)

    @pl.when(step == last)
    def _():
        store_parts(acc_ref, (p0, p1, p2, p3))


def mlp_fwd(near, far, w_up, b_up, w_down, layer, tile=512):
    half, width = near.shape
    num, hidden = 2 * half, w_up.shape[-1]
    quarter = jax.ShapeDtypeStruct((half // 2, width), BF16)
    outs = pl.pallas_call(
        mlp_fwd_kernel,
        grid=(hidden // tile,),
        in_specs=[whole((half, width)), whole((half, width)),
                  pl.BlockSpec((1, 2, width, tile), lambda f: (layer, 0, 0, f)),
                  pl.BlockSpec((1, 2, tile), lambda f: (layer, 0, f)),
                  pl.BlockSpec((1, tile, width), lambda f: (layer, f, 0))],
        out_specs=[pl.BlockSpec((2, num, tile), lambda f: (0, 0, f)),
                   pl.BlockSpec((num, tile), lambda f: (0, f))] + [whole(quarter.shape)] * 4,
        out_shape=[jax.ShapeDtypeStruct((2, num, hidden), F32),
                   jax.ShapeDtypeStruct((num, hidden), BF16)] + [quarter] * 4,
        scratch_shapes=[pltpu.VMEM((num, width), BF16), pltpu.VMEM((num, width), F32)],
        compiler_params=pltpu.CompilerParams(vmem_limit_bytes=VMEM_BYTES),
        cost_estimate=pl.CostEstimate(flops=6 * num * width * hidden, bytes_accessed=6 * width * hidden,
                                      transcendentals=num * hidden),
        name='mlp_fwd',
    )(near, far, w_up, b_up, w_down)
    return outs[0], outs[1], outs[2:]


def mlp_bwd_kernel(near_ref, far_ref, pre_ref, wu_ref, wd_ref, gp_ref, bsum_ref, p0, p1, p2, p3, gm_ref, acc_ref):
    step, last = pl.program_id(0), pl.num_programs(0) - 1

    @pl.when(step == 0)
    def _():
        join_rows(near_ref, far_ref, gm_ref)

    grad_hidden = dot_nt(gm_ref[...], wd_ref[0])
    gate, lin = pre_ref[0], pre_ref[1]
    grad_gate, grad_lin = act_grads(grad_hidden, gate, lin, jax.nn.sigmoid(gate))
    bsum_ref[0:1, :] = jnp.sum(grad_gate, axis=0, keepdims=True)
    bsum_ref[1:2, :] = jnp.sum(grad_lin, axis=0, keepdims=True)
    gp_ref[0] = grad_gate.astype(BF16)
    gp_ref[1] = grad_lin.astype(BF16)
    add_into(acc_ref, dot_nt(gp_ref[0], wu_ref[0, 0]) + dot_nt(gp_ref[1], wu_ref[0, 1]), step == 0)

    @pl.when(step == last)
    def _():
        store_parts(acc_ref, (p0, p1, p2, p3))


def mlp_bwd(near, far, pre, w_up, w_down, layer, tile=512):
    half, width = near.shape
    num, hidden = 2 * half, w_up.shape[-1]
    quarter = jax.ShapeDtypeStruct((half // 2, width), BF16)
    outs = pl.pallas_call(
        mlp_bwd_kernel,
        grid=(hidden // tile,),
        in_specs=[whole((half, width)), whole((half, width)),
                  pl.BlockSpec((2, num, tile), lambda f: (0, 0, f)),
                  pl.BlockSpec((1, 2, width, tile), lambda f: (layer, 0, 0, f)),
                  pl.BlockSpec((1, tile, width), lambda f: (layer, f, 0))],
        out_specs=[pl.BlockSpec((2, num, tile), lambda f: (0, 0, f)),
                   pl.BlockSpec((2, tile), lambda f: (0, f))] + [whole(quarter.shape)] * 4,
        out_shape=[jax.ShapeDtypeStruct((2, num, hidden), BF16),
                   jax.ShapeDtypeStruct((2, hidden), F32)] + [quarter] * 4,
        scratch_shapes=[pltpu.VMEM((num, width), BF16), pltpu.VMEM((num, width), F32)],
        compiler_params=pltpu.CompilerParams(vmem_limit_bytes=VMEM_BYTES),
        cost_estimate=pl.CostEstimate(flops=6 * num * width * hidden, bytes_accessed=6 * width * hidden,
                                      transcendentals=num * hidden),
        name='mlp_bwd',
    )(near, far, pre, w_up, w_down)
    return outs[0], outs[1], outs[2:]


def mlp_wgrad_kernel(num_alias, xt_hbm, gmn_hbm, gmf_hbm, ogn_hbm, ogf_hbm, xn_hbm, xf_hbm, after_hbm,
                     wu_ref, bu_ref, wd_ref, hid_own_ref, gp_own_ref, *rest):
    gwu_ref, gwd_ref, token_ref, x_ref, xt_ref, gm_ref, hid_ref, gp_ref, sems = rest[num_alias:]
    num = x_ref.shape[0]
    half = num // 2
    pieces = ((xn_hbm, x_ref, 0), (xf_hbm, x_ref, 1), (ogn_hbm, gm_ref, 2), (ogf_hbm, gm_ref, 3),
              (gmn_hbm, gm_ref, 0), (gmf_hbm, gm_ref, 1))
    copies = [pltpu.make_async_copy(src, dst.at[pl.ds(pos * half, half), :], sems.at[idx])
              for idx, (src, dst, pos) in enumerate(pieces)]
    copies.append(pltpu.make_async_copy(xt_hbm, xt_ref, sems.at[6]))
    first = pl.program_id(0) == 0

    @pl.when(first)
    def _():
        for copy in copies:
            copy.start()

    hid_ref[0:num, :] = hid_own_ref[...]
    gp_ref[0, 0:num, :] = gp_own_ref[0]
    gp_ref[1, 0:num, :] = gp_own_ref[1]

    @pl.when(first)
    def _():
        for copy in copies[:4]:
            copy.wait()

    gate = dot_nn(x_ref[...], wu_ref[0, 0]) + bu_ref[0, 0:1, :]
    lin = dot_nn(x_ref[...], wu_ref[0, 1]) + bu_ref[0, 1:2, :]
    grad_hidden = dot_nt(gm_ref[num:2 * num, :], wd_ref[0])
    sig = jax.nn.sigmoid(gate)
    hid_ref[num:2 * num, :] = (gate * sig * lin).astype(BF16)
    grad_gate, grad_lin = act_grads(grad_hidden, gate, lin, sig)
    gp_ref[0, num:2 * num, :] = grad_gate.astype(BF16)
    gp_ref[1, num:2 * num, :] = grad_lin.astype(BF16)

    @pl.when(first)
    def _():
        for copy in copies[4:]:
            copy.wait()

    for chan in range(2):
        gwu_ref[0, chan] = dot_nn(xt_ref[...], gp_ref[chan])
    gwd_ref[0] = dot_tn(hid_ref[...], gm_ref[...])
    token_ref[...] = jnp.zeros_like(token_ref)


def mlp_wgrad(part, layer, bufs, after, xt_all, gm_own, gm_other, x_other, w_up, b_up, w_down, hid, gp, tile=256):
    width, tokens = xt_all.shape
    num = tokens // 2
    hidden = w_up.shape[-1]
    steps = hidden // tile // WGRAD_PARTS
    base = part * steps
    any_spec = pl.BlockSpec(memory_space=pl.ANY)
    flops = 2 * width * tile * steps * (3 * num + 3 * tokens)
    outs = pl.pallas_call(
        functools.partial(mlp_wgrad_kernel, len(bufs)),
        grid=(steps,),
        in_specs=[any_spec] * 8 + [
            pl.BlockSpec((1, 2, width, tile), lambda f: (layer, 0, 0, f + base)),
            pl.BlockSpec((1, 2, tile), lambda f: (layer, 0, f + base)),
            pl.BlockSpec((1, tile, width), lambda f: (layer, f + base, 0)),
            pl.BlockSpec((num, tile), lambda f: (0, f + base)),
            pl.BlockSpec((2, num, tile), lambda f: (0, 0, f + base))] + [any_spec] * len(bufs),
        out_specs=[pl.BlockSpec((1, 2, width, tile), lambda f: (layer, 0, 0, f + base)),
                   pl.BlockSpec((1, tile, width), lambda f: (layer, f + base, 0)), whole((8, LANES))],
        out_shape=[jax.ShapeDtypeStruct(w_up.shape, F32), jax.ShapeDtypeStruct(w_down.shape, F32),
                   jax.ShapeDtypeStruct((8, LANES), F32)],
        input_output_aliases={13 + pos: pos for pos in range(len(bufs))},
        scratch_shapes=[pltpu.VMEM((num, width), BF16), pltpu.VMEM((width, tokens), BF16),
                        pltpu.VMEM((tokens, width), BF16), pltpu.VMEM((tokens, tile), BF16),
                        pltpu.VMEM((2, tokens, tile), BF16), pltpu.SemaphoreType.DMA((7,))],
        compiler_params=pltpu.CompilerParams(vmem_limit_bytes=VMEM_BYTES),
        cost_estimate=pl.CostEstimate(flops=flops, bytes_accessed=18 * width * tile * steps + 4 * tokens * width,
                                      transcendentals=num * tile * steps),
        name='mlp_wgrad',
    )(xt_all, *gm_own, *gm_other, *x_other, after, w_up, b_up, w_down, hid, gp, *bufs)
    return tuple(outs[:2]), outs[2]


def pair_weights(wq_ref, wq_pad, wp_ref, wp_pad):
    head_dim = wp_ref.shape[-2]
    wq_pad[...] = jnp.zeros_like(wq_pad)
    wp_pad[...] = jnp.zeros_like(wp_pad)
    for head in range(2):
        wp_pad[head * LANES:head * LANES + head_dim, :] = wp_ref[0, head]
        for chan in range(3):
            start = (2 * chan + head) * LANES
            wq_pad[start:start + head_dim, :] = wq_ref[0, chan, head]


def seq_rows(seq, num_seq, num_tok):
    slot_rows = num_seq * num_tok
    start = min(seq * num_tok // 16 * 16, slot_rows - SEQ_WINDOW)
    return [slot * slot_rows + start for slot in range(4)], seq * num_tok - start


def take(ref, starts, lane):
    return jnp.concatenate([ref[row:row + SEQ_WINDOW, lane:lane + LANES] for row in starts], 0).astype(BF16)


def put(ref, starts, lane, val):
    for pos, row in enumerate(starts):
        ref[row:row + SEQ_WINDOW, lane:lane + LANES] += val[pos * SEQ_WINDOW:(pos + 1) * SEQ_WINDOW, :]


def member_rows(begin, num_tok):
    row = lax.rem(lax.broadcasted_iota(jnp.int32, (4 * SEQ_WINDOW, LANES), 0), SEQ_WINDOW)
    return jnp.logical_and(row >= begin, row < begin + num_tok)


def seq_probs(query, key, keep, fill, scale):
    scores = jnp.where(keep > 0.0, dot_nt(query, key) * scale, fill)
    expd = jnp.exp(scores - jnp.max(scores, axis=-1, keepdims=True))
    return expd / jnp.sum(expd, axis=-1, keepdims=True)


def attn_fwd_kernel(num_seq, num_tok, head_dim, near_ref, far_ref, wq_ref, bq_ref, wp_ref, keep_ref, fill_ref,
                    qkv_ref, o_ref, p0, p1, p2, p3, x_ref, wq_pad, wp_pad, qkv_f32, o_f32, acc_ref):
    step, last = pl.program_id(0), pl.num_programs(0) - 1

    @pl.when(step == 0)
    def _():
        join_rows(near_ref, far_ref, x_ref)

    pair_weights(wq_ref, wq_pad, wp_ref, wp_pad)
    qkv_f32[...] = dot_nt(x_ref[...], wq_pad[...]) + bq_ref[0]
    qkv_ref[...] = qkv_f32[...].astype(BF16)
    o_f32[...] = jnp.zeros_like(o_f32)
    for seq in range(num_seq):
        starts, begin = seq_rows(seq, num_seq, num_tok)
        member = member_rows(begin, num_tok)
        for head in range(2):
            query, key, val = (take(qkv_f32, starts, (2 * chan + head) * LANES) for chan in range(3))
            probs = seq_probs(query, key, keep_ref[seq], fill_ref[seq], head_dim ** -0.5).astype(BF16)
            put(o_f32, starts, head * LANES, jnp.where(member, dot_nn(probs, val), 0.0))
    o_ref[...] = o_f32[...].astype(BF16)
    add_into(acc_ref, dot_nn(o_ref[...], wp_pad[...]), step == 0)

    @pl.when(step == last)
    def _():
        store_parts(acc_ref, (p0, p1, p2, p3))


def attn_specs(layer, wq, wp, keep):
    head_dim, width = wp.shape[-2:]
    return [pl.BlockSpec((1, 3, 2, head_dim, width), lambda f: (layer, 0, f, 0, 0)),
            pl.BlockSpec((1, 2, head_dim, width), lambda f: (layer, f, 0, 0)), whole(keep.shape), whole(keep.shape)]


def attn_fwd(near, far, wq, bq, wp, keep, fill, layer, num_seq):
    half, width = near.shape
    num, (heads, head_dim) = 2 * half, wp.shape[1:3]
    quarter = jax.ShapeDtypeStruct((half // 2, width), BF16)
    spec_wq, spec_wp, spec_keep, spec_fill = attn_specs(layer, wq, wp, keep)
    outs = pl.pallas_call(
        functools.partial(attn_fwd_kernel, num_seq, half // 2 // num_seq, head_dim),
        grid=(heads // 2,),
        in_specs=[whole((half, width)), whole((half, width)), spec_wq,
                  pl.BlockSpec((1, 1, 6 * LANES), lambda f: (f, 0, 0)), spec_wp, spec_keep, spec_fill],
        out_specs=[pl.BlockSpec((num, 6 * LANES), lambda f: (0, f)),
                   pl.BlockSpec((num, 2 * LANES), lambda f: (0, f))] + [whole(quarter.shape)] * 4,
        out_shape=[jax.ShapeDtypeStruct((num, 3 * heads * LANES), BF16),
                   jax.ShapeDtypeStruct((num, heads * LANES), BF16)] + [quarter] * 4,
        scratch_shapes=[pltpu.VMEM((num, width), BF16), pltpu.VMEM((6 * LANES, width), BF16),
                        pltpu.VMEM((2 * LANES, width), BF16), pltpu.VMEM((num, 6 * LANES), F32),
                        pltpu.VMEM((num, 2 * LANES), F32), pltpu.VMEM((num, width), F32)],
        compiler_params=pltpu.CompilerParams(vmem_limit_bytes=VMEM_BYTES),
        cost_estimate=pl.CostEstimate(flops=16 * num * width * heads * head_dim, bytes_accessed=8 * num * width,
                                      transcendentals=4 * heads * num * num // num_seq),
        name='attn_fwd',
    )(near, far, wq, bq, wp, keep, fill)
    return outs[0], outs[1], outs[2:]


def attn_bwd_kernel(num_seq, num_tok, head_dim, gn_ref, gf_ref, xn_ref, xf_ref, wq_ref, wp_ref, keep_ref, fill_ref,
                    qkv_ref, o_ref, gwq_ref, gwp_ref, bsum_ref, p0, p1, p2, p3,
                    g_ref, x_ref, wq_pad, wp_pad, qkv_f32, do_f32, dqkv_f32, dqkv_bf, acc_ref):
    step, last = pl.program_id(0), pl.num_programs(0) - 1

    @pl.when(step == 0)
    def _():
        join_rows(gn_ref, gf_ref, g_ref)
        join_rows(xn_ref, xf_ref, x_ref)

    pair_weights(wq_ref, wq_pad, wp_ref, wp_pad)
    do_f32[...] = dot_nt(g_ref[...], wp_pad[...])
    qkv_f32[...] = qkv_ref[...].astype(F32)
    dqkv_f32[...] = jnp.zeros_like(dqkv_f32)
    scale = head_dim ** -0.5
    for seq in range(num_seq):
        starts, begin = seq_rows(seq, num_seq, num_tok)
        member = member_rows(begin, num_tok)
        for head in range(2):
            query, key, val = (take(qkv_f32, starts, (2 * chan + head) * LANES) for chan in range(3))
            grad_o = jnp.where(member, take(do_f32, starts, head * LANES), jnp.zeros((), BF16))
            probs = seq_probs(query, key, keep_ref[seq], fill_ref[seq], scale)
            grad_probs = dot_nt(grad_o, val)
            put(dqkv_f32, starts, (4 + head) * LANES, dot_tn(probs.astype(BF16), grad_o))
            delta = jnp.sum(grad_probs * probs, axis=-1, keepdims=True)
            grad_scores = (probs * (grad_probs - delta) * scale).astype(BF16)
            put(dqkv_f32, starts, head * LANES, dot_nn(grad_scores, key))
            put(dqkv_f32, starts, (2 + head) * LANES, dot_tn(grad_scores, query))
    bsum_ref[0] = jnp.sum(dqkv_f32[...], axis=0, keepdims=True)
    dqkv_bf[...] = dqkv_f32[...].astype(BF16)
    grad_wq = dot_tn(dqkv_bf[...], x_ref[...])
    grad_wp = dot_tn(o_ref[...], g_ref[...])
    for head in range(2):
        gwp_ref[head] = grad_wp[head * LANES:head * LANES + head_dim, :].astype(BF16)
        for chan in range(3):
            start = (2 * chan + head) * LANES
            gwq_ref[chan, head] = grad_wq[start:start + head_dim, :].astype(BF16)
    add_into(acc_ref, dot_nn(dqkv_bf[...], wq_pad[...]), step == 0)

    @pl.when(step == last)
    def _():
        store_parts(acc_ref, (p0, p1, p2, p3))


def attn_bwd(g_near, g_far, near, far, wq, wp, keep, fill, qkv, attn, layer, num_seq):
    half, width = near.shape
    num, (heads, head_dim) = 2 * half, wp.shape[1:3]
    quarter = jax.ShapeDtypeStruct((half // 2, width), BF16)
    outs = pl.pallas_call(
        functools.partial(attn_bwd_kernel, num_seq, half // 2 // num_seq, head_dim),
        grid=(heads // 2,),
        in_specs=[whole((half, width))] * 4 + attn_specs(layer, wq, wp, keep) + [
            pl.BlockSpec((num, 6 * LANES), lambda f: (0, f)), pl.BlockSpec((num, 2 * LANES), lambda f: (0, f))],
        out_specs=[pl.BlockSpec((3, 2, head_dim, width), lambda f: (0, f, 0, 0)),
                   pl.BlockSpec((2, head_dim, width), lambda f: (f, 0, 0)),
                   pl.BlockSpec((1, 1, 6 * LANES), lambda f: (f, 0, 0))] + [whole(quarter.shape)] * 4,
        out_shape=[jax.ShapeDtypeStruct((3, heads, head_dim, width), BF16),
                   jax.ShapeDtypeStruct((heads, head_dim, width), BF16),
                   jax.ShapeDtypeStruct((heads // 2, 1, 6 * LANES), F32)] + [quarter] * 4,
        scratch_shapes=[pltpu.VMEM((num, width), BF16), pltpu.VMEM((num, width), BF16),
                        pltpu.VMEM((6 * LANES, width), BF16), pltpu.VMEM((2 * LANES, width), BF16),
                        pltpu.VMEM((num, 6 * LANES), F32), pltpu.VMEM((num, 2 * LANES), F32),
                        pltpu.VMEM((num, 6 * LANES), F32), pltpu.VMEM((num, 6 * LANES), BF16),
                        pltpu.VMEM((num, width), F32)],
        compiler_params=pltpu.CompilerParams(vmem_limit_bytes=VMEM_BYTES),
        cost_estimate=pl.CostEstimate(flops=32 * num * width * heads * head_dim, bytes_accessed=16 * num * width,
                                      transcendentals=4 * heads * num * num // num_seq),
        name='attn_bwd',
    )(g_near, g_far, near, far, wq, wp, keep, fill, qkv, attn)
    return outs[0], outs[1], outs[2], outs[3:]


def pair_sum_kernel(num_alias, a_ref, b_ref, *rest):
    rest[num_alias][0] = a_ref[...].astype(F32) + b_ref[...].astype(F32)


def pair_sum(own, other, layer, num_blocks, buf):
    lead, (rows, width) = own.shape[0], own.shape[1:]
    num_alias = 0 if buf is None else 1
    return pl.pallas_call(
        functools.partial(pair_sum_kernel, num_alias),
        grid=(lead,),
        in_specs=[pl.BlockSpec((1, rows, width), lambda f: (f, 0, 0))] * 2 + [
            pl.BlockSpec(memory_space=pl.ANY)] * num_alias,
        out_specs=pl.BlockSpec((1, 1, rows, width), lambda f: (layer, f, 0, 0)),
        out_shape=jax.ShapeDtypeStruct((num_blocks,) + own.shape, F32),
        input_output_aliases={2: 0} if num_alias else {},
        cost_estimate=pl.CostEstimate(flops=own.size, bytes_accessed=8 * own.size, transcendentals=0),
        name='pair_sum',
    )(own, other, *([] if buf is None else [buf]))


def block_fwd(x_loc, masks, prm, layer, params, packed, num_seq):
    (norm1_gain, norm1_bias, w_qkv, b_qkv, w_proj, b_proj, layer_scale1,
     norm2_gain, norm2_bias, w_up, b_up, w_down, b_down, layer_scale2) = prm
    wq, bq = packed
    normed, hat_one, std_one = norm_fwd(x_loc, norm1_gain, norm1_bias)
    near, far = gather_rows(normed)
    qkv, attn, parts = attn_fwd(near, far, wq, bq[layer], params[4], *masks, layer, num_seq)
    attn_sum = scatter_rows(parts) + b_proj
    x_mid = (x_loc.astype(F32) + layer_scale1 * attn_sum).astype(BF16)
    normed2, hat_two, std_two = norm_fwd(x_mid, norm2_gain, norm2_bias)
    near2, far2 = gather_rows(normed2)
    pre, hid, parts = mlp_fwd(near2, far2, params[9], params[10], params[11], layer)
    mlp_sum = scatter_rows(parts) + b_down
    x_out = (x_mid.astype(F32) + layer_scale2 * mlp_sum).astype(BF16)
    saved = (hat_one, std_one, near, far, qkv, attn, attn_sum, hat_two, std_two, near2, far2, pre, hid, mlp_sum)
    return x_out, saved


def block_bwd(grad_x, saved, masks, prm, layer, params, packed, bufs, pending, num_seq):
    (norm1_gain, norm1_bias, w_qkv, b_qkv, w_proj, b_proj, layer_scale1,
     norm2_gain, norm2_bias, w_up, b_up, w_down, b_down, layer_scale2) = prm
    (hat_one, std_one, near, far, qkv, attn, attn_sum, hat_two, std_two, near2, far2, pre, hid, mlp_sum) = saved
    grad_res = grad_x.astype(F32)
    grad_ls2 = jnp.sum(grad_res * mlp_sum, axis=0)
    grad_mlp = layer_scale2 * grad_res
    grad_b_down = jnp.sum(grad_mlp, axis=0)
    gm_near, gm_far = gather_rows(grad_mlp.astype(BF16))
    gp, grad_b_up, parts = mlp_bwd(gm_near, gm_far, pre, params[9], params[11], layer)
    on_near, on_far = gather_other_dp(near2, far2)
    og_near, og_far = gather_other_dp(gm_near, gm_far)
    pending = tuple(after_token(val, (og_near, og_far)) for val in pending)
    exchanged = [(val, to_dp(val)) for val in pending]
    xt_all = jnp.concatenate([near2, far2, on_near, on_far], 0).T
    state = [bufs, 0]

    def wgrad_part(after):
        state[0], token = mlp_wgrad(state[1], layer, state[0], after, xt_all, (gm_near, gm_far), (og_near, og_far),
                                    (on_near, on_far), params[9], params[10], params[11], hid, gp)
        state[1] += 1
        return token

    grad_normed2 = scatter_rows(parts, wgrad_part)
    grad_from2, grad_n2g, grad_n2b = norm_bwd(grad_normed2, hat_two, std_two, norm2_gain)
    grad_mid = grad_res + grad_from2
    grad_ls1 = jnp.sum(grad_mid * attn_sum, axis=0)
    grad_attn_out = layer_scale1 * grad_mid
    grad_b_proj = jnp.sum(grad_attn_out, axis=0)
    ga_near, ga_far = gather_rows(grad_attn_out.astype(BF16), wgrad_part)
    grad_w_qkv, grad_w_proj, grad_b_qkv, parts = attn_bwd(ga_near, ga_far, near, far, packed[0], params[4], *masks,
                                                          qkv, attn, layer, num_seq)
    grad_normed = scatter_rows(parts, wgrad_part)
    grad_from1, grad_n1g, grad_n1b = norm_bwd(grad_normed, hat_one, std_one, norm1_gain)
    grad_in = (grad_mid + grad_from1).astype(BF16)
    shared = jnp.stack([grad_n1g, grad_n1b, grad_b_proj, grad_ls1, grad_n2g, grad_n2b, grad_b_down, grad_ls2])
    pending = (grad_w_qkv.reshape((-1,) + grad_w_qkv.shape[2:]), grad_w_proj)
    return grad_in, state[0], exchanged, pending, (shared, grad_b_qkv, grad_b_up)


def solution(mesh):
    small_spec = P()
    act_spec = P('dp', 'tp', None)
    param_specs = (small_spec, small_spec, P(None, None, None, 'tp', None), P(None, None, 'tp', None),
                   P(None, 'tp', None, None), small_spec, small_spec, small_spec, small_spec,
                   P(None, None, None, 'tp'), P(None, None, 'tp'), P(None, 'tp', None), small_spec, small_spec)

    def device_fn(tokens, grad_y, valid_len, *params):
        num_blocks = params[0].shape[0]
        num_seq, num_tok, width = tokens.shape
        heads, head_dim = params[3].shape[2:]
        slots = lax.axis_index('tp') ^ jnp.arange(4)
        keep, fill = [], []
        for seq in range(num_seq):
            begin = seq_rows(seq, num_seq, num_tok)[1]
            local = jnp.arange(SEQ_WINDOW) - begin
            member = jnp.broadcast_to((local >= 0) & (local < num_tok), (4, SEQ_WINDOW))
            valid = member & (slots[:, None] * num_tok + local[None, :] < valid_len[seq])
            keep.append(valid.reshape(1, -1).astype(F32))
            fill.append(jnp.where(member, NEG_BIG, LOW_FILL).reshape(1, -1).astype(F32))
        masks = (jnp.stack(keep), jnp.stack(fill))
        wq = params[2].transpose(0, 1, 3, 4, 2)
        bq = jnp.pad(params[3], ((0, 0), (0, 0), (0, 0), (0, LANES - head_dim)))
        bq = bq.reshape(num_blocks, 3, heads // 2, 2 * LANES).transpose(0, 2, 1, 3)
        bq = bq.reshape(num_blocks, heads // 2, 1, 6 * LANES)
        packed = (wq, bq)
        x_cur = tokens.reshape(num_seq * num_tok, width)
        saved_all = []
        for layer in range(num_blocks):
            x_cur, saved = block_fwd(x_cur, masks, tuple(arr[layer] for arr in params), layer, params, packed, num_seq)
            saved_all.append(saved)
        grad_cur = grad_y.reshape(num_seq * num_tok, width)
        grads = [None] * num_blocks
        bufs, pending, attn_bufs = (), (), (None, None)

        def collect(exchanged, layer, attn_bufs):
            return tuple(pair_sum(own, other, layer, num_blocks, buf)
                         for (own, other), buf in zip(exchanged, attn_bufs))

        for layer in reversed(range(num_blocks)):
            grad_cur, bufs, exchanged, pending, grads[layer] = block_bwd(
                grad_cur, saved_all[layer], masks, tuple(arr[layer] for arr in params), layer, params, packed, bufs,
                pending, num_seq)
            if exchanged:
                attn_bufs = collect(exchanged, layer + 1, attn_bufs)
        attn_bufs = collect([(val, to_dp(val)) for val in pending], 0, attn_bufs)
        w_qkv = attn_bufs[0].reshape(num_blocks, 3, heads, head_dim, width).transpose(0, 1, 4, 2, 3)
        shared, b_qkv, b_up = (jnp.stack(vals) for vals in zip(*grads))
        b_qkv = b_qkv.reshape(num_blocks, heads // 2, 3, 2, LANES).transpose(0, 2, 1, 3, 4)
        b_qkv = b_qkv.reshape(num_blocks, 3, heads, LANES)[..., :head_dim]
        b_qkv, b_up = b_qkv + to_dp(b_qkv), b_up + to_dp(b_up)
        shared = sum_all(shared.reshape(-1, width)).reshape(num_blocks, -1, width).transpose(1, 0, 2)
        return (x_cur.reshape(tokens.shape), grad_cur.reshape(tokens.shape), shared[0], shared[1], w_qkv, b_qkv,
                attn_bufs[1], shared[2], shared[3], shared[4], shared[5], bufs[0], b_up, bufs[1], shared[6], shared[7])

    return jax.shard_map(device_fn, mesh=mesh, in_specs=(act_spec, act_spec, P('dp')) + param_specs,
                         out_specs=(act_spec, act_spec) + param_specs, check_vma=False)
```
